32 devices in a mesh: groups: 1, ep: 32 (over z, y, x, core).
Axes of the slice: x: 2, y: 2, z: 4, core: 2. Of those that a mesh axis runs over, the one named last changes fastest.
Arguments:
- tokens: bfloat16 [2048, 2880], P(('groups', 'ep')), may hold values from -6 to 6
- routes: int32 [2048, 4], P(('groups', 'ep')), may hold values from 0 to 7, all different within a row; in each aligned block of 64 rows (0 to 63, 64 to 127, ...) at most 36 rows name the same one
- norm_gain: bfloat16 [2880], replicated, may hold values from 0.25 to 1.75
- router_weight: bfloat16 [2880, 8], replicated, may hold values from -0.02734375 to 0.02734375
- gate_up_weight: bfloat16 [32, 2880, 720], P('ep'), may hold values from -0.109375 to 0.109375
- down_weight: bfloat16 [32, 360, 2880], P('ep'), may hold values from -0.15625 to 0.15625
Outputs:
- mixed: bfloat16 [2048, 2880], P(('groups', 'ep'))
The draws below stay inside these ranges and needn't reach their ends.
Inputs may be any that keep to these rules, and one draw needn't show every extreme that they name: `routes`: in each aligned block of 64 rows (the rows of one device), no expert is named by more than 36 rows; in some blocks one expert is named by exactly 36 rows. A row names 4 different experts.
All inputs are finite; a program needn't handle non-finite values.
Results may differ from the reference program's by a relative error of at most 0.005.
Values may be sent and summed in bfloat16 or wider, within the bound.
A program may use at most 128 MiB of HBM per device.

```python
import math
import jax
import jax.numpy as jnp
import numpy as np
from jax import lax

D = 2880
FF_WIN = 1440
TOP = 4
SHARD = 4
TOK_DEV = 64
EXPERTS = 8
FF_DEV = 360
CAP = 36
TOKENS = 2048
N_EP = 32


def level_of(own_key, extent, pieces, least, high):
    def one(axis_at, shards_of):
        steps = jax.random.uniform(jax.random.fold_in(jax.random.fold_in(own_key, 6), axis_at), (shards_of,), jnp.float32, least / len(pieces), high / len(pieces))
        return jnp.repeat(jnp.exp(steps), extent[axis_at] // shards_of).reshape((-1,) + (1,) * (len(extent) - axis_at - 1))

    level = one(*pieces[0])
    for cut in pieces[1:]:
        level = level * one(*cut)
    return level


def assign_block(own_key, own, number, rows, number_of, top, reach, slope):
    order = jax.random.permutation(own_key, number_of)
    heavy_load, usual = load_shares(number_of, rows * top, reach, slope, True), load_shares(number_of, rows * top, reach, slope, False)
    places = jnp.arange(number_of)

    def named(lengths, turn):
        used = int((lengths > 0).sum())
        fixed = max(1, used // 4)
        shifted = fixed + (places - fixed + turn * (used - fixed)) % max(1, number_of - fixed)
        return jnp.zeros((number_of,), jnp.int32).at[order[jnp.where(places < fixed, places, shifted)]].set(jnp.asarray(lengths, jnp.int32))

    lengths = jnp.where(number % 4 == 0, named(heavy_load, number // 4), named(usual, number - number // 4 - 1))
    mixed = jax.random.permutation(jax.random.fold_in(own, 3), number_of)
    source_of, receiver = mixed[0:number_of // 2 * 2:2], mixed[1:number_of // 2 * 2:2]
    margin = jnp.minimum(lengths[source_of] - 1, reach - lengths[receiver]) // 2
    margin = jnp.where((source_of == order[0]) | (receiver == order[0]) | (lengths[receiver] == 0), 0, jnp.maximum(margin, 0))
    shifted = jax.random.randint(jax.random.fold_in(own, 4), (number_of // 2,), 0, 1 << 20) % (margin + 1)
    lengths = lengths.at[source_of].add(-shifted).at[receiver].add(shifted)
    members = jnp.searchsorted(jnp.cumsum(lengths), jnp.arange(rows * top), side="right").astype(jnp.int32)
    table = members.reshape(top, rows).T
    table = table[jax.random.permutation(jax.random.fold_in(own, 1), rows)]
    turn = jax.random.randint(jax.random.fold_in(own, 2), (rows, 1), 0, top)
    return jnp.take_along_axis(table, (jnp.arange(top)[None, :] + turn) % top, axis=1)


def load_shares(number_of, total, reach, lean, full):
    portions = [(1 << 20) // math.isqrt(standing ** lean) + 1 for standing in range(1, number_of + 1)]
    largest = reach if full else min(reach, max(-(-total // number_of), total * portions[0] // sum(portions)))
    least = 1 if total - largest >= number_of - 1 else 0
    given, rest = [largest] + [least] * (number_of - 1), total - largest - least * (number_of - 1)
    while rest > 0:
        free = [i for i in range(1, number_of) if given[i] < largest] or [i for i in range(1, number_of) if given[i] < reach]
        whole, left = sum([portions[i] for i in free]), rest
        for i in free:
            more = min(reach - given[i], max(1, left * portions[i] // whole), rest)
            given[i] = given[i] + more
            rest = rest - more
    return np.array(given)


def centred(stream_key, shape, width, reach, cuts=(), held_as=jnp.bfloat16):
    values = width * jax.random.normal(stream_key, shape, jnp.float32)
    if cuts:
        values = values * level_of(stream_key, shape, cuts, -0.22, 0.18)
    return jnp.clip(values, -reach, reach).astype(held_as)


def setup_inputs(seed: int = 0, part: int = 0) -> dict:
    streams_of = jax.random.split(jax.random.key(seed), 7)
    own_keys = jax.random.split(jax.random.fold_in(streams_of[6], part), 7)
    tokens = centred(own_keys[0], (TOKENS, D), 1.0, 6.0, ((0, 32),))
    routes_keys = jax.random.split(jax.random.fold_in(own_keys[1], 1), TOKENS // TOK_DEV)
    routes_turns = jax.random.permutation(jax.random.fold_in(own_keys[1], 3), TOKENS // TOK_DEV)
    routes = jax.vmap(lambda own, number: assign_block(jax.random.fold_in(own_keys[1], 2), own, number, TOK_DEV, EXPERTS, TOP, CAP, 2))(routes_keys, routes_turns).reshape((TOKENS, TOP))
    norm_gain = jnp.clip(1.0 + 0.15 * jax.random.normal(streams_of[2], (D,), jnp.float32), 0.25, 1.75).astype(jnp.bfloat16)
    router_weight = centred(streams_of[3], (D, EXPERTS), (16 * D) ** -0.5, 0.02734375)
    gate_up_weight = centred(streams_of[4], (EXPERTS * SHARD, D, 2 * FF_DEV), D ** -0.5, 0.109375, ((0, 32),))
    down_weight = centred(streams_of[5], (EXPERTS * SHARD, FF_DEV, D), FF_WIN ** -0.5, 0.15625, ((0, 32),))
    return dict(tokens=tokens, routes=routes, norm_gain=norm_gain, router_weight=router_weight, gate_up_weight=gate_up_weight, down_weight=down_weight)


def reference(tokens, routes, norm_gain, router_weight, gate_up_weight, down_weight):
    stream = tokens.astype(jnp.float32)
    mean_square = lax.optimization_barrier(jnp.mean(stream * stream, axis=-1, keepdims=True))
    normed = (stream * lax.rsqrt(mean_square + 1e-05) * norm_gain.astype(jnp.float32)).astype(jnp.bfloat16)
    logits = jnp.dot(normed, router_weight, preferred_element_type=jnp.float32)
    expert_ids = jnp.arange(EXPERTS, dtype=jnp.int32)
    onehot = routes[:, :, None] == expert_ids[None, None, :]
    chosen = lax.optimization_barrier(jnp.sum(jnp.where(onehot, logits[:, None, :], jnp.float32(0.0)), axis=-1))
    expo = jnp.exp(chosen)
    route_prob = expo / lax.optimization_barrier(jnp.sum(expo, axis=-1, keepdims=True))
    flat_hits = onehot.astype(jnp.int32).reshape(N_EP, TOK_DEV * TOP, EXPERTS)
    rank_before = jnp.cumsum(flat_hits, axis=1) - flat_hits
    slot_index = lax.optimization_barrier(jnp.sum(flat_hits * rank_before, axis=-1)).reshape(TOKENS, TOP).astype(jnp.int32)
    block_ids = (jnp.arange(TOKENS, dtype=jnp.int32) // TOK_DEV)[:, None]
    position = (block_ids * CAP + slot_index).astype(jnp.int32)
    values = jnp.broadcast_to(normed[:, None, :], (TOKENS, TOP, D))
    buffer = jnp.zeros((EXPERTS, N_EP * CAP, D), jnp.bfloat16).at[routes, position].set(values)
    gate_up_all = gate_up_weight.reshape(EXPERTS, SHARD, D, 2 * FF_DEV)
    down_all = down_weight.reshape(EXPERTS, SHARD, FF_DEV, D)

    def one_expert(operands):
        rows, gate_up_part, down_part = operands
        total = jnp.zeros((N_EP * CAP, D), jnp.float32)
        for member in range(SHARD):
            hidden = jnp.dot(rows, gate_up_part[member], preferred_element_type=jnp.float32)
            gate_part = hidden[:, :FF_DEV]
            up_part = hidden[:, FF_DEV:]
            activated = ((up_part + 1.0) * gate_part * jax.nn.sigmoid(1.702 * gate_part)).astype(jnp.bfloat16)
            partial_value = jnp.dot(activated, down_part[member], preferred_element_type=jnp.float32).astype(jnp.bfloat16)
            total = total + partial_value.astype(jnp.float32)
        return total
    expert_sum = lax.map(one_expert, (buffer, gate_up_all, down_all))
    mixture = jnp.zeros((TOKENS, D), jnp.float32)
    for choice_k in range(TOP):
        picked = expert_sum[routes[:, choice_k], position[:, choice_k]]
        mixture = mixture + route_prob[:, choice_k:choice_k + 1] * picked
    return (stream + mixture).astype(jnp.bfloat16)
```

```python
import functools

import jax
import jax.numpy as jnp
from jax import lax
from jax.experimental import pallas as pl
from jax.experimental.pallas import tpu as pltpu
from jax.sharding import PartitionSpec as P

SHARD = 4
LANES = 128
MESH = pl.DeviceIdType.MESH
ABSENT = -1024.0


def cuts(width, weights):
    tiles = width // LANES
    total = sum(weights)
    edges = [0]
    run = 0
    for w in weights:
        run += w
        edges.append(max(edges[-1] + 1, round(tiles * run / total)))
    edges[-1] = tiles
    return [(a * LANES, (b - a) * LANES) for a, b in zip(edges[:-1], edges[1:])]


def moe_kernel(
    planes, cols, capacity, fan_in, fan_out,
    tokens, routes, gain, router, gate_up_hbm, down_hbm,
    out,
    gate_up_raw, down_raw, gate_up, down, rank_all, tok_all, rows_in, other_in,
    hidden, act, part, mate_in, cross_in, pair, mix, mix_in,
    w_sem, rank_sem, z_sem, y_sem, x_sem, c_sem, c2_sem, x2_sem, y2_sem, z2_sem,
):
    f32 = jnp.float32
    bf16 = jnp.bfloat16
    me = lax.axis_index("ep")
    group = me // SHARD
    member = me % SHARD
    core = member % 2
    half = member // 2
    plane = group // cols
    col = group % cols
    experts = router.shape[1]
    toks, width = tokens.shape
    wide = tok_all.shape[1]
    ff = down_raw.shape[0]
    ffp = act.shape[1]
    sect = planes * capacity

    def device(p, c, h, k):
        return (p * cols + c) * SHARD + h * 2 + k

    mate = device(plane, col, half, 1 - core)
    across = device(plane, col, 1 - half, core)
    beside = device(plane, 1 - col, half, core)
    turns = sorted(range(1, planes), key=lambda r: min(r, planes - r))
    column = [device((plane + r) % planes, col, half, core) for r in turns]
    near = [mate, across, beside] + column

    loads = [
        pltpu.make_async_copy(gate_up_hbm, gate_up_raw, w_sem.at[0]),
        pltpu.make_async_copy(down_hbm, down_raw, w_sem.at[1]),
    ]
    for copy in loads:
        copy.start()

    barrier = pltpu.get_barrier_semaphore()
    for other in near:
        pl.semaphore_signal(barrier, inc=1, device_id={"ep": other}, device_id_type=MESH)

    def send(src, dst, sems, slot, target):
        return pltpu.make_async_remote_copy(
            src_ref=src, dst_ref=dst, send_sem=sems.at[0, slot], recv_sem=sems.at[1, slot],
            device_id={"ep": target}, device_id_type=MESH,
        )

    lane_e = lax.broadcasted_iota(jnp.int32, (toks, experts), 1)
    chosen = routes[...]
    hit = jnp.zeros((toks, experts), f32)
    for k in range(chosen.shape[1]):
        hit = hit + jnp.where(chosen[:, k : k + 1] == lane_e, 1.0, 0.0)
    lower = lax.broadcasted_iota(jnp.int32, (toks, toks), 1) < lax.broadcasted_iota(
        jnp.int32, (toks, toks), 0
    )
    rank = jnp.dot(
        jnp.where(lower, 1.0, 0.0).astype(bf16), hit.astype(bf16), preferred_element_type=f32
    )
    rank = jnp.where(hit > 0.0, rank, ABSENT)

    def lanes_from(value, base):
        select = lax.broadcasted_iota(jnp.int32, (experts, LANES), 1) == (
            lax.broadcasted_iota(jnp.int32, (experts, LANES), 0) + base
        )
        return jnp.dot(
            value.astype(bf16), jnp.where(select, 1.0, 0.0).astype(bf16),
            preferred_element_type=f32,
        )

    mine = pl.ds(pl.multiple_of(plane * toks, toks), toks)
    rank_all[mine, :] = lanes_from(rank, 0).astype(bf16)

    stream = tokens[...].astype(f32)
    mean_square = jnp.mean(stream * stream, axis=-1, keepdims=True)
    normed = (stream * lax.rsqrt(mean_square + 1e-05) * gain[...].astype(f32)).astype(bf16)
    tok_all[mine, wide - LANES : wide] = jnp.zeros((toks, LANES), bf16)
    tok_all[mine, 0:width] = normed

    pl.semaphore_wait(barrier, len(near))

    rank_copies = [
        send(rank_all.at[mine], rank_all.at[mine], rank_sem, i, column[i])
        for i in range(planes - 1)
    ]
    for copy in rank_copies:
        copy.start()
    z_copies = [
        [
            send(
                tok_all.at[mine, pl.ds(f0, fw)], tok_all.at[mine, pl.ds(f0, fw)],
                z_sem, k * (planes - 1) + i, column[i],
            )
            for i in range(planes - 1)
        ]
        for k, (f0, fw) in enumerate(fan_in)
    ]
    last = len(fan_in) - 1
    for k in range(last):
        for copy in z_copies[k]:
            copy.start()

    logits = jnp.dot(normed, router[...], preferred_element_type=f32)
    expo = jnp.where(hit > 0.0, jnp.exp(logits), 0.0)
    prob = expo / jnp.sum(expo, axis=-1, keepdims=True)
    high = prob.astype(bf16)
    low = (prob - high.astype(f32)).astype(bf16)
    base = LANES - (wide - width)
    tail = lanes_from(high, base) + lanes_from(low, base + experts)
    tok_all[mine, wide - LANES : wide] = (
        tok_all[mine, wide - LANES : wide].astype(f32) + tail
    ).astype(bf16)
    for copy in z_copies[last]:
        copy.start()

    expert = group
    expert_other = plane * cols + (1 - col)
    count = planes * toks
    for copy in rank_copies:
        copy.wait_recv()
    pick = lax.broadcasted_iota(jnp.int32, (16, LANES), 1) == jnp.where(
        lax.broadcasted_iota(jnp.int32, (16, LANES), 0) == 0, expert, expert_other
    )
    rank_rows = lax.dot_general(
        jnp.where(pick, 1.0, 0.0).astype(bf16), rank_all[...],
        (((1,), (1,)), ((), ())), preferred_element_type=f32,
    )
    block_of = (lax.broadcasted_iota(jnp.int32, (1, count), 1) // toks * capacity).astype(f32)
    slot_rows = lax.broadcasted_iota(jnp.int32, (sect, count), 0).astype(f32)
    gather = jnp.concatenate(
        [
            jnp.where(rank_rows[i : i + 1, :] + block_of == slot_rows, 1.0, 0.0).astype(bf16)
            for i in range(2)
        ],
        axis=0,
    )

    def section(j):
        return pl.ds(j * sect, sect)

    y_copies = [
        send(
            other_in.at[:, pl.ds(f0, fw)], rows_in.at[section(1), pl.ds(f0, fw)],
            y_sem, k, beside,
        )
        for k, (f0, fw) in enumerate(fan_in)
    ]
    x_copies = [
        [
            send(
                rows_in.at[section(j), pl.ds(f0, fw)], rows_in.at[section(2 + j), pl.ds(f0, fw)],
                x_sem, 2 * k + j, across,
            )
            for j in range(2)
        ]
        for k, (f0, fw) in enumerate(fan_in)
    ]
    c_copies = [
        [
            send(
                rows_in.at[section(j), pl.ds(f0, fw)], rows_in.at[section(4 + j), pl.ds(f0, fw)],
                c_sem, 4 * k + j, mate,
            )
            for j in range(4)
        ]
        for k, (f0, fw) in enumerate(fan_in)
    ]
    chunk = 2 * sect
    groups_in = 8 * sect // chunk

    def prepare():
        loads[0].wait()
        tile = 96
        steps = width // tile

        def move(i, carry):
            r = pl.ds(pl.multiple_of(i * tile, tile), tile)
            both = gate_up_raw[r, :].astype(f32)
            zero = jnp.zeros((tile, ffp - ff), f32)
            gate_up[r, 0:ffp] = jnp.concatenate([both[:, 0:ff], zero], axis=1).astype(bf16)
            gate_up[r, ffp : 2 * ffp] = jnp.concatenate([both[:, ff : 2 * ff], zero], axis=1).astype(
                bf16
            )
            return carry

        lax.fori_loop(0, steps, move, 0)
        gate_up[width:wide, :] = jnp.zeros((wide - width, 2 * ffp), bf16)
        loads[1].wait()
        down[:, wide - LANES : wide] = jnp.zeros((ffp, LANES), bf16)
        down[ff - ff % 16 : ffp, :] = jnp.zeros((ffp - ff + ff % 16, wide), bf16)
        down[0:ff, 0:width] = down_raw[...]

    def expand(k):
        f0, fw = fan_in[k]
        for j in range(4):
            c_copies[k][j].wait_recv()

        def one(g, carry):
            r = pl.ds(pl.multiple_of(g * chunk, chunk), chunk)
            value = jnp.dot(
                rows_in[r, f0 : f0 + fw], gate_up[f0 : f0 + fw, :], preferred_element_type=f32
            )
            if k == 0:
                hidden[r, :] = value
            else:
                hidden[r, :] += value
            return carry

        lax.fori_loop(0, groups_in, one, 0)

    def relay(k):
        for j in range(2):
            x_copies[k][j].wait_recv()
            c_copies[k][2 + j].start()

    for k, (f0, fw) in enumerate(fan_in):
        for copy in z_copies[k]:
            copy.wait_recv()
        value = jnp.dot(gather, tok_all[:, f0 : f0 + fw], preferred_element_type=f32).astype(bf16)
        other_in[:, f0 : f0 + fw] = value[sect : 2 * sect]
        rows_in[0:sect, f0 : f0 + fw] = value[0:sect]
        y_copies[k].start()
        x_copies[k][0].start()
        c_copies[k][0].start()
        if k == 0:
            prepare()
        y_copies[k].wait_recv()
        x_copies[k][1].start()
        c_copies[k][1].start()
        if k >= 1:
            relay(k - 1)
        if k >= 2:
            expand(k - 2)
    if last >= 1:
        expand(last - 1)
    relay(last)
    expand(last)

    lane_t = lax.broadcasted_iota(jnp.int32, (chunk, LANES), 1)
    is_prob = (lane_t == base + expert) | (lane_t == base + experts + expert)

    def activate(g, carry):
        r = pl.ds(pl.multiple_of(g * chunk, chunk), chunk)
        tails = rows_in[r, wide - LANES : wide].astype(f32)
        weight = jnp.sum(jnp.where(is_prob, tails, 0.0), axis=-1, keepdims=True)
        gate_part = hidden[r, 0:ffp]
        up_part = hidden[r, ffp : 2 * ffp]
        act[r, :] = (
            (up_part + 1.0) * gate_part * jax.nn.sigmoid(1.702 * gate_part) * weight
        ).astype(bf16)
        return carry

    lax.fori_loop(0, groups_in, activate, 0)

    lane_r = lax.broadcasted_iota(jnp.int32, (count, LANES), 1)
    ranks = rank_all[...].astype(f32)
    spot = [
        jnp.sum(jnp.where(lane_r == e, ranks, 0.0), axis=-1, keepdims=True)
        for e in (expert, expert_other)
    ]
    block_at = (lax.broadcasted_iota(jnp.int32, (count, 1), 0) // toks * capacity).astype(f32)
    lane_s = lax.broadcasted_iota(jnp.int32, (count, 2 * sect), 1)
    at = jnp.where(lane_s < sect, spot[0] + block_at, spot[1] + block_at + float(sect))
    keep = jnp.where(lane_s < sect, spot[0], spot[1]) >= 0.0
    scatter = jnp.where(keep & (at == lane_s.astype(f32)), 1.0, 0.0).astype(bf16)

    c2 = [
        [
            send(
                part.at[section(4 + j), pl.ds(f0, fw)], mate_in.at[section(j), pl.ds(f0, fw)],
                c2_sem, 4 * k + j, mate,
            )
            for j in range(4)
        ]
        for k, (f0, fw) in enumerate(fan_out)
    ]
    x2 = [
        [
            send(
                part.at[section(2 + j), pl.ds(f0, fw)], cross_in.at[section(j), pl.ds(f0, fw)],
                x2_sem, 2 * k + j, across,
            )
            for j in range(2)
        ]
        for k, (f0, fw) in enumerate(fan_out)
    ]
    y2 = [
        send(
            part.at[section(1), pl.ds(f0, fw)], pair.at[section(1), pl.ds(f0, fw)],
            y2_sem, k, beside,
        )
        for k, (f0, fw) in enumerate(fan_out)
    ]
    z2 = [
        [
            send(
                mix.at[
                    pl.ds(pl.multiple_of((plane + turns[i]) % planes * toks, toks), toks),
                    pl.ds(f0, fw),
                ],
                mix_in.at[i, :, pl.ds(f0, fw)],
                z2_sem, k * (planes - 1) + i, column[i],
            )
            for i in range(planes - 1)
        ]
        for k, (f0, fw) in enumerate(fan_out)
    ]

    def contract(k):
        f0, fw = fan_out[k]

        def one(i, carry):
            g = groups_in - 1 - i
            r = pl.ds(pl.multiple_of(g * chunk, chunk), chunk)
            part[r, f0 : f0 + fw] = jnp.dot(
                act[r, :], down[:, f0 : f0 + fw], preferred_element_type=f32
            ).astype(bf16)
            return carry

        lax.fori_loop(0, groups_in, one, 0)
        for j in (2, 3, 0, 1):
            c2[k][j].start()

    def add_mate(k):
        f0, fw = fan_out[k]
        for j in (2, 3, 0, 1):
            c2[k][j].wait_recv()
            a = part[j * sect : (j + 1) * sect, f0 : f0 + fw].astype(f32)
            b = mate_in[j * sect : (j + 1) * sect, f0 : f0 + fw].astype(f32)
            part[j * sect : (j + 1) * sect, f0 : f0 + fw] = (a + b).astype(bf16)
            if j >= 2:
                x2[k][j - 2].start()

    def add_across(k):
        f0, fw = fan_out[k]
        x2[k][1].wait_recv()
        a = part[sect : 2 * sect, f0 : f0 + fw].astype(f32)
        b = cross_in[sect : 2 * sect, f0 : f0 + fw].astype(f32)
        part[sect : 2 * sect, f0 : f0 + fw] = (a + b).astype(bf16)
        y2[k].start()
        x2[k][0].wait_recv()
        a = part[0:sect, f0 : f0 + fw].astype(f32)
        b = cross_in[0:sect, f0 : f0 + fw].astype(f32)
        pair[0:sect, f0 : f0 + fw] = (a + b).astype(bf16)

    def to_tokens(k):
        f0, fw = fan_out[k]
        y2[k].wait_recv()
        mix[:, f0 : f0 + fw] = jnp.dot(
            scatter, pair[:, f0 : f0 + fw], preferred_element_type=f32
        ).astype(bf16)
        for copy in z2[k]:
            copy.start()

    def finish(k):
        f0, fw = fan_out[k]
        f1 = min(f0 + fw, width)
        for copy in z2[k]:
            copy.wait_recv()
        total = mix[mine, f0:f1].astype(f32)
        for i in range(planes - 1):
            total = total + mix_in[i, :, f0:f1].astype(f32)
        out[:, f0:f1] = (tokens[:, f0:f1].astype(f32) + total).astype(bf16)

    ends = len(fan_out)
    for k in range(ends + 3):
        if k < ends:
            contract(k)
        if 1 <= k <= ends:
            add_mate(k - 1)
        if 2 <= k <= ends + 1:
            add_across(k - 2)
        if 3 <= k <= ends + 2:
            to_tokens(k - 3)
    for k in range(ends):
        finish(k)

    for copy in rank_copies + y_copies + y2:
        copy.wait_send()
    for many in z_copies + x_copies + c_copies + c2 + x2 + z2:
        for copy in many:
            copy.wait_send()


def shards(tokens, routes, norm_gain, router_weight, gate_up_weight, down_weight):
    toks, width = tokens.shape
    top_count = routes.shape[1]
    experts = router_weight.shape[1]
    devices = lax.axis_size("ep")
    groups = devices // SHARD
    cols = 2
    planes = groups // cols
    ff = down_weight.shape[1]
    capacity = min(toks, SHARD * (17 * toks * top_count // (16 * experts * SHARD) + 1))
    wide = -(-(width + 2 * experts) // LANES) * LANES
    ffp = -(-ff // LANES) * LANES
    sect = planes * capacity
    fan_in = cuts(wide, [2, 4, 6, 6, 3, 2])
    fan_out = cuts(wide, [3, 6, 6, 5, 3])
    n_in, n_out = len(fan_in), len(fan_out)
    bf16 = jnp.bfloat16
    vmem = pl.BlockSpec(memory_space=pltpu.VMEM)
    hbm = pl.BlockSpec(memory_space=pl.ANY)
    dma = lambda n: pltpu.SemaphoreType.DMA((2, n))
    return pl.pallas_call(
        functools.partial(moe_kernel, planes, cols, capacity, fan_in, fan_out),
        out_shape=jax.ShapeDtypeStruct((toks, width), bf16),
        in_specs=[vmem, vmem, vmem, vmem, hbm, hbm],
        out_specs=vmem,
        scratch_shapes=[
            pltpu.VMEM((width, 2 * ff), bf16),
            pltpu.VMEM((ff, width), bf16),
            pltpu.VMEM((wide, 2 * ffp), bf16),
            pltpu.VMEM((ffp, wide), bf16),
            pltpu.VMEM((planes * toks, LANES), bf16),
            pltpu.VMEM((planes * toks, wide), bf16),
            pltpu.VMEM((8 * sect, wide), bf16),
            pltpu.VMEM((sect, wide), bf16),
            pltpu.VMEM((8 * sect, 2 * ffp), jnp.float32),
            pltpu.VMEM((8 * sect, ffp), bf16),
            pltpu.VMEM((8 * sect, wide), bf16),
            pltpu.VMEM((4 * sect, wide), bf16),
            pltpu.VMEM((2 * sect, wide), bf16),
            pltpu.VMEM((2 * sect, wide), bf16),
            pltpu.VMEM((planes * toks, wide), bf16),
            pltpu.VMEM((planes - 1, toks, wide), bf16),
            pltpu.SemaphoreType.DMA((2,)),
            dma(planes - 1),
            dma(n_in * (planes - 1)),
            dma(n_in),
            dma(2 * n_in),
            dma(4 * n_in),
            dma(4 * n_out),
            dma(2 * n_out),
            dma(n_out),
            dma(n_out * (planes - 1)),
        ],
        compiler_params=pltpu.CompilerParams(
            collective_id=0, has_side_effects=True, vmem_limit_bytes=63 * 1024 * 1024
        ),
    )(
        tokens,
        routes,
        norm_gain.reshape(1, width),
        router_weight,
        gate_up_weight[0],
        down_weight[0],
    )


def solution(mesh):
    in_specs = (
        P(("groups", "ep"), None),
        P(("groups", "ep"), None),
        P(),
        P(),
        P("ep", None, None),
        P("ep", None, None),
    )
    out_specs = P(("groups", "ep"), None)
    return jax.shard_map(shards, mesh=mesh, in_specs=in_specs, out_specs=out_specs, check_vma=False)
```

```python
import functools

import jax
import jax.numpy as jnp
from jax import lax
from jax.experimental import pallas as pl
from jax.experimental.pallas import tpu as pltpu
from jax.sharding import PartitionSpec as P

SHARD = 4
LANES = 128
MESH = pl.DeviceIdType.MESH
ABSENT = -1024.0
FAN_IN = ((2, "direct"), (3, "narrow"), (3, "narrow"), (4, "narrow"), (5, "narrow"), (3, "wide"), (3, "wide"))
FAN_OUT = ((1, "narrow"), (2, "wide"), (4, "wide"), (6, "narrow"), (5, "narrow"), (5, "direct"))
ORDER = (
    "S1", "S2", "S0", "W5", "R2", "L", "S3", "W6",
    "R1", "G2", "S4", "G0", "G1", "R3", "Y2", "Y1",
    "G3", "S6", "R4", "SX6", "X1", "X2", "G4", "SX5",
    "R6", "RX6", "G6", "S5", "Y4", "C1", "RX5", "GX6",
    "SC", "C2", "Y0", "GX5", "Y3", "R5", "X4", "G5",
    "X0", "YX6", "Y6", "C4", "YX5", "C6", "X3", "C0",
    "Y5", "C3", "C5", "A", "e0", "e1", "e3", "m0",
    "m1", "e2", "m3", "m2", "x0", "t1", "tx1", "t2",
    "e4", "e5", "x3", "m4", "t0", "r1", "m5", "rx1",
    "r2", "r0", "tx2", "t3", "rx2", "x4", "f0", "r3",
    "x5", "t4", "r4", "xl2", "f3", "f2", "t5", "xl1",
    "f1", "f4", "f5",
)


def cuts(width, plan):
    tiles = width // LANES
    total = sum(weight for weight, _ in plan)
    pieces = [max(1, tiles * weight // total) for weight, _ in plan]
    while sum(pieces) != tiles:
        step = 1 if sum(pieces) < tiles else -1
        gap = [step * (weight * tiles / total - piece) for piece, (weight, _) in zip(pieces, plan)]
        pieces[gap.index(max(gap))] += step
    wide_at = sum(p for p, (_, kind) in zip(pieces, plan) if kind != "wide") * LANES
    narrow_at = 0
    spans = []
    for piece, (_, kind) in zip(pieces, plan):
        size = piece * LANES
        if kind == "wide":
            spans.append((wide_at, size, kind))
            wide_at += size
        else:
            spans.append((narrow_at, size, kind))
            narrow_at += size
    return spans


def wide_span(spans):
    wide = [(f0, fw) for f0, fw, kind in spans if kind == "wide"]
    return min(f0 for f0, _ in wide), sum(fw for _, fw in wide)


def moe_kernel(
    planes, cols, capacity, fan_in, fan_out,
    tokens, routes, gain, router, gate_up_hbm, down_hbm,
    out,
    gate_up, down_raw, down, rank_all, rank_x, tok_all, tok_x, rows_in, other_in,
    hidden, act, part, mate_in, cross_in, pair, pair_x, mix, mix_x, mix_in, mix_x_in, total,
    final_x, final_x_in,
    w_sem, rank_sem, w_x_sem, z_sem, y_sem, x_sem, c_sem, c2_sem, x2_sem, y2_sem, z2_sem, w_x2_sem,
):
    f32 = jnp.float32
    bf16 = jnp.bfloat16
    me = lax.axis_index("ep")
    group = me // SHARD
    member = me % SHARD
    core = member % 2
    half = member // 2
    plane = group // cols
    col = group % cols
    experts = router.shape[0]
    toks, width = tokens.shape
    wide = tok_all.shape[1]
    ff = down_raw.shape[0]
    ffp = act.shape[1]
    sect = planes * capacity
    count = planes * toks
    reach = planes - 1
    dirs = (1, -1)
    in_x = wide_span(fan_in)[0]
    out_x = wide_span(fan_out)[0]

    def device(p, c, h, k):
        return (p * cols + c) * SHARD + h * 2 + k

    mate = device(plane, col, half, 1 - core)
    across = device(plane, col, 1 - half, core)
    beside = device(plane, 1 - col, half, core)
    turns = sorted(range(1, planes), key=lambda r: min(r, planes - r))
    column = [device((plane + r) % planes, col, half, core) for r in turns]
    column_x = [device((plane + r) % planes, col, 1 - half, core) for r in turns]
    near = [mate, across, beside] + column + column_x

    def inside(p):
        return (p >= 0) & (p < planes)

    def clip(p):
        return jnp.clip(p, 0, planes - 1)

    for i in range(2):
        gate_up[(i + 1) * ffp - LANES : (i + 1) * ffp, :] = jnp.zeros((LANES, width), bf16)
    loads = [
        pltpu.make_async_copy(
            gate_up_hbm.at[pl.ds(i * ff, ff)], gate_up.at[pl.ds(i * ffp, ff)], w_sem.at[i]
        )
        for i in range(2)
    ] + [pltpu.make_async_copy(down_hbm, down_raw, w_sem.at[2])]
    for copy in loads:
        copy.start()

    barrier = pltpu.get_barrier_semaphore()
    for other in near:
        pl.semaphore_signal(barrier, inc=1, device_id={"ep": other}, device_id_type=MESH)

    def send(src, dst, sems, slot, target):
        return pltpu.make_async_remote_copy(
            src_ref=src, dst_ref=dst, send_sem=sems.at[0, slot], recv_sem=sems.at[1, slot],
            device_id={"ep": target}, device_id_type=MESH,
        )

    def block(p):
        return pl.ds(pl.multiple_of(p * toks, toks), toks)

    row_e = lax.broadcasted_iota(jnp.int32, (experts, toks), 0)
    chosen = routes[...]
    hit_rows = jnp.zeros((experts, toks), f32)
    for k in range(chosen.shape[0]):
        hit_rows = hit_rows + jnp.where(chosen[k : k + 1, :] == row_e, 1.0, 0.0)
    at_col = lax.broadcasted_iota(jnp.int32, (toks, toks), 1)
    at_row = lax.broadcasted_iota(jnp.int32, (toks, toks), 0)

    def by_token(mask):
        return lax.dot_general(
            jnp.where(mask, 1.0, 0.0).astype(bf16), hit_rows.astype(bf16),
            (((1,), (1,)), ((), ())), preferred_element_type=f32,
        )

    hit = by_token(at_col == at_row)
    rank = jnp.where(hit > 0.0, by_token(at_col < at_row), ABSENT)

    def lanes_from(value, base):
        select = lax.broadcasted_iota(jnp.int32, (experts, LANES), 1) == (
            lax.broadcasted_iota(jnp.int32, (experts, LANES), 0) + base
        )
        return jnp.dot(
            value.astype(bf16), jnp.where(select, 1.0, 0.0).astype(bf16),
            preferred_element_type=f32,
        )

    mine = block(plane)
    rank_all[mine, :] = lanes_from(rank, 0).astype(bf16)

    stream = tokens[...].astype(f32)
    mean_square = jnp.mean(stream * stream, axis=-1, keepdims=True)
    normed = (stream * lax.rsqrt(mean_square + 1e-05) * gain[...].astype(f32)[None, :]).astype(bf16)
    tok_all[mine, wide - LANES : wide] = jnp.zeros((toks, LANES), bf16)
    tok_all[mine, 0:width] = normed

    pl.semaphore_wait(barrier, len(near))

    rank_copies = [
        send(rank_all.at[mine], rank_all.at[mine], rank_sem, i, column[i]) for i in range(reach)
    ]
    rank_x_copies = [
        send(rank_all.at[mine], rank_x.at[mine], rank_sem, reach + i, target)
        for i, target in enumerate([across] + column_x)
    ]

    lanes_of = {}
    for k, (f0, fw, kind) in enumerate(fan_in):
        lanes_of[k] = [(tok_all, f0, fw, 2 * k)]
        if kind == "wide":
            lanes_of[k].append((tok_x, f0 - in_x, fw, 2 * k + 1))

    def z_copy(k, lane, s, d):
        ref, a, fw, at = lanes_of[k][lane]
        relayed = d >= 3 and fan_in[k][2] != "direct"
        source = block(clip(plane - s * (d - 1))) if relayed else mine
        target = clip(plane + (s if relayed else s * d))
        view = ref.at[source, pl.ds(a, fw)]
        slot = (at * 2 + (s + 1) // 2) * reach + d - 1
        return send(view, view, z_sem, slot, device(target, col, half, core))

    def z_sends(k, d, s):
        if d >= 3 and fan_in[k][2] != "direct":
            return inside(plane - s * (d - 1)) & inside(plane + s)
        return inside(plane + s * d)

    def z_start(k, lane):
        direct = fan_in[k][2] == "direct"
        for d in range(reach if direct else min(2, reach), 0, -1):
            for s in dirs:
                pl.when(z_sends(k, d, s))(z_copy(k, lane, s, d).start)

    def z_relay(k, lane):
        if fan_in[k][2] == "direct":
            return
        for d in range(3, planes):
            for s in dirs:

                @pl.when(z_sends(k, d, s))
                def _():
                    z_copy(k, lane, s, d - 1).wait_recv()
                    z_copy(k, lane, s, d).start()

    def z_arrive(k, lane):
        for d in range(1, planes):
            for s in dirs:
                come = inside(plane - s * d)
                if d >= 2 and d < reach and fan_in[k][2] != "direct":
                    come = come & ~inside(plane + s)
                pl.when(come)(z_copy(k, lane, s, d).wait_recv)

    def z_drain(k, lane):
        for d in range(1, planes):
            for s in dirs:
                pl.when(z_sends(k, d, s))(z_copy(k, lane, s, d).wait_send)

    for copy in rank_copies + rank_x_copies:
        copy.start()
    w_x_copies = {}
    for k, (f0, fw, kind) in enumerate(fan_in):
        if kind == "wide":
            w_x_copies[k] = send(
                tok_all.at[mine, pl.ds(f0, fw)], tok_x.at[mine, pl.ds(f0 - in_x, fw)],
                w_x_sem, k, across,
            )
    base = LANES - (wide - width)

    def add_prob():
        logits = lax.dot_general(
            normed, router[...], (((1,), (1,)), ((), ())), preferred_element_type=f32
        )
        expo = jnp.where(hit > 0.0, jnp.exp(logits), 0.0)
        prob = expo / jnp.sum(expo, axis=-1, keepdims=True)
        high = prob.astype(bf16)
        low = (prob - high.astype(f32)).astype(bf16)
        tail = lanes_from(high, base) + lanes_from(low, base + experts)
        tok_all[mine, wide - LANES : wide] = (
            tok_all[mine, wide - LANES : wide].astype(f32) + tail
        ).astype(bf16)

    expert = group
    expert_other = plane * cols + (1 - col)

    def gather_of(ranks):
        pick = lax.broadcasted_iota(jnp.int32, (16, LANES), 1) == jnp.where(
            lax.broadcasted_iota(jnp.int32, (16, LANES), 0) == 0, expert, expert_other
        )
        rank_rows = lax.dot_general(
            jnp.where(pick, 1.0, 0.0).astype(bf16), ranks[...],
            (((1,), (1,)), ((), ())), preferred_element_type=f32,
        )
        block_of = (lax.broadcasted_iota(jnp.int32, (1, count), 1) // toks * capacity).astype(f32)
        slot_rows = lax.broadcasted_iota(jnp.int32, (sect, count), 0).astype(f32)
        return jnp.concatenate(
            [
                jnp.where(rank_rows[i : i + 1, :] + block_of == slot_rows, 1.0, 0.0).astype(bf16)
                for i in range(2)
            ],
            axis=0,
        )

    def scatter_of(ranks_ref):
        lane_r = lax.broadcasted_iota(jnp.int32, (count, LANES), 1)
        ranks = ranks_ref[...].astype(f32)
        spot = [
            jnp.sum(jnp.where(lane_r == e, ranks, 0.0), axis=-1, keepdims=True)
            for e in (expert, expert_other)
        ]
        block_at = (lax.broadcasted_iota(jnp.int32, (count, 1), 0) // toks * capacity).astype(f32)
        lane_s = lax.broadcasted_iota(jnp.int32, (count, 2 * sect), 1)
        at = jnp.where(lane_s < sect, spot[0] + block_at, spot[1] + block_at + float(sect))
        keep = jnp.where(lane_s < sect, spot[0], spot[1]) >= 0.0
        return jnp.where(keep & (at == lane_s.astype(f32)), 1.0, 0.0).astype(bf16)

    def section(j):
        return pl.ds(j * sect, sect)

    y_copies = [
        [
            send(
                other_in.at[section(i), pl.ds(f0, fw)],
                rows_in.at[section(1 + 2 * i), pl.ds(f0, fw)],
                y_sem, 2 * k + i, beside,
            )
            for i in range(2 if kind == "wide" else 1)
        ]
        for k, (f0, fw, kind) in enumerate(fan_in)
    ]
    x_copies = [
        [
            send(
                rows_in.at[section(j), pl.ds(f0, fw)], rows_in.at[section(2 + j), pl.ds(f0, fw)],
                x_sem, 2 * k + j, across,
            )
            for j in range(0 if kind == "wide" else 2)
        ]
        for k, (f0, fw, kind) in enumerate(fan_in)
    ]
    c_copies = [
        [
            send(
                rows_in.at[section(j), pl.ds(f0, fw)], rows_in.at[section(4 + j), pl.ds(f0, fw)],
                c_sem, 4 * k + j, mate,
            )
            for j in range(4)
        ]
        for k, (f0, fw, _) in enumerate(fan_in)
    ]
    chunk = 2 * sect
    groups_in = 8 * sect // chunk

    def prepare():
        for copy in loads:
            copy.wait()
        down[:, wide - LANES : wide] = jnp.zeros((ffp, LANES), bf16)
        down[ff - ff % 16 : ffp, :] = jnp.zeros((ffp - ff + ff % 16, wide), bf16)
        down[0:ff, 0:width] = down_raw[...]

    def cross_first(k):
        w_x_copies[k].wait_recv()
        z_start(k, 1)

    gathers = {}

    def gather_rows(k):
        f0, fw, kind = fan_in[k]
        if 0 not in gathers:
            for copy in rank_copies:
                copy.wait_recv()
            gathers[0] = gather_of(rank_all)
        z_arrive(k, 0)
        value = jnp.dot(
            gathers[0], tok_all[:, f0 : f0 + fw], preferred_element_type=f32
        ).astype(bf16)
        other_in[0:sect, f0 : f0 + fw] = value[sect : 2 * sect]
        rows_in[0:sect, f0 : f0 + fw] = value[0:sect]
        y_copies[k][0].start()
        if kind != "wide":
            x_copies[k][0].start()
        c_copies[k][0].start()

    def gather_rows_x(k):
        f0, fw, kind = fan_in[k]
        if 1 not in gathers:
            for copy in rank_x_copies:
                copy.wait_recv()
            gathers[1] = gather_of(rank_x)
        z_arrive(k, 1)
        a = f0 - in_x
        value = jnp.dot(gathers[1], tok_x[:, a : a + fw], preferred_element_type=f32).astype(bf16)
        other_in[sect : 2 * sect, f0 : f0 + fw] = value[sect : 2 * sect]
        rows_in[2 * sect : 3 * sect, f0 : f0 + fw] = value[0:sect]
        y_copies[k][1].start()
        c_copies[k][2].start()

    def from_beside(k, i):
        y_copies[k][i].wait_recv()
        if fan_in[k][2] != "wide":
            x_copies[k][1].start()
        c_copies[k][1 + 2 * i].start()

    def from_across(k):
        for j, copy in enumerate(x_copies[k]):
            copy.wait_recv()
            c_copies[k][2 + j].start()

    done_in = []

    def expand(k):
        f0, fw, _ = fan_in[k]
        f1 = min(f0 + fw, width)
        for j in range(4):
            c_copies[k][j].wait_recv()
        first = not done_in
        if first:
            prepare()
        done_in.append(k)

        def one(g, carry):
            r = pl.ds(pl.multiple_of(g * chunk, chunk), chunk)
            value = lax.dot_general(
                rows_in[r, f0:f1], gate_up[:, f0:f1], (((1,), (1,)), ((), ())),
                preferred_element_type=f32,
            )
            if first:
                hidden[r, :] = value
            else:
                hidden[r, :] += value
            return carry

        lax.fori_loop(0, groups_in, one, 0)

    n_in = len(fan_in)
    lane_t = lax.broadcasted_iota(jnp.int32, (chunk, LANES), 1)
    is_prob = (lane_t == base + expert) | (lane_t == base + experts + expert)

    def activate_group(g, carry):
        r = pl.ds(pl.multiple_of(g * chunk, chunk), chunk)
        tails = rows_in[r, wide - LANES : wide].astype(f32)
        weight = jnp.sum(jnp.where(is_prob, tails, 0.0), axis=-1, keepdims=True)
        gate_part = hidden[r, 0:ffp]
        up_part = hidden[r, ffp : 2 * ffp]
        act[r, :] = (
            (up_part + 1.0) * gate_part * jax.nn.sigmoid(1.702 * gate_part) * weight
        ).astype(bf16)
        return carry

    def activate():
        lax.fori_loop(0, groups_in, activate_group, 0)

    n_out = len(fan_out)
    c2 = [
        [
            send(
                part.at[section(4 + j), pl.ds(f0, fw)], mate_in.at[section(j), pl.ds(f0, fw)],
                c2_sem, 4 * k + j, mate,
            )
            for j in range(4)
        ]
        for k, (f0, fw, _) in enumerate(fan_out)
    ]
    x2 = [
        [
            send(
                part.at[section(2 + j), pl.ds(f0, fw)], cross_in.at[section(j), pl.ds(f0, fw)],
                x2_sem, 2 * k + j, across,
            )
            for j in range(0 if kind == "wide" else 2)
        ]
        for k, (f0, fw, kind) in enumerate(fan_out)
    ]
    y2 = [
        [send(part.at[section(1), pl.ds(f0, fw)], pair.at[section(1), pl.ds(f0, fw)], y2_sem, 2 * k, beside)]
        for k, (f0, fw, _) in enumerate(fan_out)
    ]
    lanes_to = {}
    for k, (f0, fw, kind) in enumerate(fan_out):
        lanes_to[k] = [(mix, mix_in, f0, fw, 2 * k)]
        if kind == "wide":
            a = f0 - out_x
            y2[k].append(
                send(
                    part.at[section(3), pl.ds(f0, fw)], pair_x.at[section(1), pl.ds(a, fw)],
                    y2_sem, 2 * k + 1, beside,
                )
            )
            lanes_to[k].append((mix_x, mix_x_in, a, fw, 2 * k + 1))
    w_x2 = {
        k: send(
            final_x.at[:, pl.ds(f0 - out_x, fw)], final_x_in.at[:, pl.ds(f0 - out_x, fw)],
            w_x2_sem, k, across,
        )
        for k, (f0, fw, kind) in enumerate(fan_out)
        if kind == "wide"
    }

    def z2_copy(k, lane, s, d):
        src, dst, a, fw, at = lanes_to[k][lane]
        relayed = d >= 3 and fan_out[k][2] != "direct"
        target = clip(plane - (s if relayed else s * d))
        spot = (s + 1) // 2 * reach + d - 1
        return send(
            src.at[block(clip(plane - s * d)), pl.ds(a, fw)], dst.at[spot, :, pl.ds(a, fw)],
            z2_sem, at * 2 * reach + spot, device(target, col, half, core),
        )

    def z2_adds(k, s, d):
        if d < 2 or d >= reach or fan_out[k][2] == "direct":
            return None
        return inside(plane + s)

    def z2_start(k, lane):
        for d in range(reach, 0, -1):
            for s in dirs:
                go = inside(plane - s * d)
                adds = z2_adds(k, s, d)
                if adds is not None:
                    go = go & ~adds
                pl.when(go)(z2_copy(k, lane, s, d).start)

    def z2_relay(k, lane):
        src, dst, a, fw, _ = lanes_to[k][lane]
        for d in range(reach - 1, 1, -1):
            for s in dirs:
                adds = z2_adds(k, s, d)
                if adds is None:
                    continue

                @pl.when(inside(plane - s * d) & adds)
                def _():
                    z2_copy(k, lane, s, d + 1).wait_recv()
                    rows = block(clip(plane - s * d))
                    spot = (s + 1) // 2 * reach + d
                    src[rows, a : a + fw] = (
                        src[rows, a : a + fw].astype(f32) + dst[spot, :, a : a + fw].astype(f32)
                    ).astype(bf16)
                    z2_copy(k, lane, s, d).start()

    def z2_sum(k, lane):
        src, dst, a, fw, _ = lanes_to[k][lane]
        total[:, 0:fw] = src[mine, a : a + fw].astype(f32)
        far = reach if fan_out[k][2] == "direct" else min(2, reach)
        for d in range(1, far + 1):
            for s in dirs:

                @pl.when(inside(plane + s * d))
                def _():
                    z2_copy(k, lane, s, d).wait_recv()
                    spot = (s + 1) // 2 * reach + d - 1
                    total[:, 0:fw] += dst[spot, :, a : a + fw].astype(f32)

    def z2_drain(k, lane):
        for d in range(1, planes):
            for s in dirs:
                pl.when(inside(plane - s * d))(z2_copy(k, lane, s, d).wait_send)

    def contract(k):
        f0, fw, _ = fan_out[k]

        def one(i, carry):
            g = groups_in - 1 - i
            r = pl.ds(pl.multiple_of(g * chunk, chunk), chunk)
            part[r, f0 : f0 + fw] = jnp.dot(
                act[r, :], down[:, f0 : f0 + fw], preferred_element_type=f32
            ).astype(bf16)
            return carry

        lax.fori_loop(0, groups_in, one, 0)
        for j in (3, 2, 1, 0):
            c2[k][j].start()

    def plus(a, b):
        return (a.astype(f32) + b.astype(f32)).astype(bf16)

    def add_mate(k):
        f0, fw, kind = fan_out[k]
        for j in (3, 1, 2, 0) if kind == "wide" else (3, 2, 1, 0):
            c2[k][j].wait_recv()
            r = slice(j * sect, (j + 1) * sect)
            value = plus(part[r, f0 : f0 + fw], mate_in[r, f0 : f0 + fw])
            if kind != "wide":
                part[r, f0 : f0 + fw] = value
                if j >= 2:
                    x2[k][j - 2].start()
            elif j % 2 == 1:
                part[r, f0 : f0 + fw] = value
                y2[k][j // 2].start()
            elif j == 0:
                pair[0:sect, f0 : f0 + fw] = value
            else:
                pair_x[0:sect, f0 - out_x : f0 - out_x + fw] = value

    def add_across(k):
        f0, fw, kind = fan_out[k]
        x2[k][1].wait_recv()
        r = slice(sect, 2 * sect)
        part[r, f0 : f0 + fw] = plus(part[r, f0 : f0 + fw], cross_in[r, f0 : f0 + fw])
        y2[k][0].start()

    scatters = {}

    def place():
        scatters[0] = scatter_of(rank_all)
        scatters[1] = scatter_of(rank_x)

    def to_tokens(k):
        f0, fw, kind = fan_out[k]
        if kind != "wide":
            x2[k][0].wait_recv()
            r = slice(0, sect)
            pair[r, f0 : f0 + fw] = plus(part[r, f0 : f0 + fw], cross_in[r, f0 : f0 + fw])
        y2[k][0].wait_recv()
        mix[:, f0 : f0 + fw] = jnp.dot(
            scatters[0], pair[:, f0 : f0 + fw], preferred_element_type=f32
        ).astype(bf16)
        z2_start(k, 0)

    def to_tokens_x(k):
        f0, fw, kind = fan_out[k]
        y2[k][1].wait_recv()
        a = f0 - out_x
        mix_x[:, a : a + fw] = jnp.dot(
            scatters[1], pair_x[:, a : a + fw], preferred_element_type=f32
        ).astype(bf16)
        z2_start(k, 1)

    def cross_last(k):
        f0, fw, kind = fan_out[k]
        a = f0 - out_x
        z2_sum(k, 1)
        final_x[:, a : a + fw] = total[:, 0:fw].astype(bf16)
        w_x2[k].start()

    def finish(k):
        f0, fw, kind = fan_out[k]
        f1 = min(f0 + fw, width)
        z2_sum(k, 0)
        value = tokens[:, f0:f1].astype(f32) + total[:, 0 : f1 - f0]
        if kind == "wide":
            w_x2[k].wait_recv()
            value = value + final_x_in[:, f0 - out_x : f1 - out_x].astype(f32)
        out[:, f0:f1] = value.astype(bf16)

    steps = {
        "L": add_prob,
        "A": activate,
        "SC": place,
        "W": lambda k: w_x_copies[k].start(),
        "S": lambda k: z_start(k, 0),
        "R": lambda k: z_relay(k, 0),
        "G": gather_rows,
        "SX": cross_first,
        "RX": lambda k: z_relay(k, 1),
        "GX": gather_rows_x,
        "Y": lambda k: from_beside(k, 0),
        "YX": lambda k: from_beside(k, 1),
        "X": from_across,
        "C": expand,
        "e": contract,
        "m": add_mate,
        "x": add_across,
        "t": to_tokens,
        "tx": to_tokens_x,
        "r": lambda k: z2_relay(k, 0),
        "rx": lambda k: z2_relay(k, 1),
        "xl": cross_last,
        "f": finish,
    }
    for word in ORDER:
        name = word.rstrip("0123456789")
        steps[name](*([int(word[len(name) :])] if word != name else []))

    for copy in rank_copies + rank_x_copies + list(w_x_copies.values()) + list(w_x2.values()):
        copy.wait_send()
    for many in y_copies + x_copies + c_copies + c2 + x2 + y2:
        for copy in many:
            copy.wait_send()
    for k in range(n_in):
        for lane in range(len(lanes_of[k])):
            z_drain(k, lane)
    for k in range(n_out):
        for lane in range(len(lanes_to[k])):
            z2_drain(k, lane)


def shards(tokens, routes, norm_gain, router_weight, gate_up_weight, down_weight):
    toks, width = tokens.shape
    top_count = routes.shape[1]
    experts = router_weight.shape[1]
    devices = lax.axis_size("ep")
    groups = devices // SHARD
    cols = 2
    planes = groups // cols
    ff = down_weight.shape[1]
    capacity = min(toks, SHARD * (17 * toks * top_count // (16 * experts * SHARD) + 1))
    wide = -(-(width + 2 * experts) // LANES) * LANES
    ffp = -(-ff // LANES) * LANES
    sect = planes * capacity
    count = planes * toks
    fan_in = cuts(wide, FAN_IN)
    fan_out = cuts(wide, FAN_OUT)
    n_in, n_out = len(fan_in), len(fan_out)
    wide_in, wide_out = wide_span(fan_in)[1], wide_span(fan_out)[1]
    most = max(fw for _, fw, _ in fan_out)
    spots = 2 * (planes - 1)
    bf16 = jnp.bfloat16
    vmem = pl.BlockSpec(memory_space=pltpu.VMEM)
    hbm = pl.BlockSpec(memory_space=pl.ANY)
    dma = lambda n: pltpu.SemaphoreType.DMA((2, n))
    return pl.pallas_call(
        functools.partial(moe_kernel, planes, cols, capacity, fan_in, fan_out),
        out_shape=jax.ShapeDtypeStruct((toks, width), bf16),
        in_specs=[vmem, vmem, vmem, vmem, hbm, hbm],
        out_specs=vmem,
        scratch_shapes=[
            pltpu.VMEM((2 * ffp, width), bf16),
            pltpu.VMEM((ff, width), bf16),
            pltpu.VMEM((ffp, wide), bf16),
            pltpu.VMEM((count, LANES), bf16),
            pltpu.VMEM((count, LANES), bf16),
            pltpu.VMEM((count, wide), bf16),
            pltpu.VMEM((count, wide_in), bf16),
            pltpu.VMEM((8 * sect, wide), bf16),
            pltpu.VMEM((2 * sect, wide), bf16),
            pltpu.VMEM((8 * sect, 2 * ffp), jnp.float32),
            pltpu.VMEM((8 * sect, ffp), bf16),
            pltpu.VMEM((8 * sect, wide), bf16),
            pltpu.VMEM((4 * sect, wide), bf16),
            pltpu.VMEM((2 * sect, wide), bf16),
            pltpu.VMEM((2 * sect, wide), bf16),
            pltpu.VMEM((2 * sect, wide_out), bf16),
            pltpu.VMEM((count, wide), bf16),
            pltpu.VMEM((count, wide_out), bf16),
            pltpu.VMEM((spots, toks, wide), bf16),
            pltpu.VMEM((spots, toks, wide_out), bf16),
            pltpu.VMEM((toks, most), jnp.float32),
            pltpu.VMEM((toks, wide_out), bf16),
            pltpu.VMEM((toks, wide_out), bf16),
            pltpu.SemaphoreType.DMA((3,)),
            dma(2 * planes - 1),
            dma(n_in),
            dma(n_in * 2 * spots),
            dma(2 * n_in),
            dma(2 * n_in),
            dma(4 * n_in),
            dma(4 * n_out),
            dma(2 * n_out),
            dma(2 * n_out),
            dma(n_out * 2 * spots),
            dma(n_out),
        ],
        compiler_params=pltpu.CompilerParams(
            collective_id=0, has_side_effects=True, vmem_limit_bytes=63 * 1024 * 1024
        ),
    )(
        tokens,
        routes.T,
        norm_gain,
        router_weight.T,
        gate_up_weight[0].T,
        down_weight[0],
    )


def solution(mesh):
    in_specs = (
        P(("groups", "ep"), None),
        P(("groups", "ep"), None),
        P(),
        P(),
        P("ep", None, None),
        P("ep", None, None),
    )
    out_specs = P(("groups", "ep"), None)
    return jax.shard_map(shards, mesh=mesh, in_specs=in_specs, out_specs=out_specs, check_vma=False)
```
